32 devices in a mesh: path: 4 (over y, core), fsdp: 8 (over z, x).
Axes of the slice: x: 2, y: 2, z: 4, core: 2. Of those that a mesh axis runs over, the one named last changes fastest.
Arguments:
- input_activation_matrix: bfloat16 [4, 1536, 2048], P('path', 'fsdp'), may hold values from -6 to 6
- output_sensitivity: bfloat16 [4, 1536, 2048], P('path', 'fsdp'), may hold values from -12 to 12
- trajectory_initial_parameters: bfloat16 [4, 8, 1024, 4096], P('path', None, 'fsdp'), may hold values from -6 to 6
- trajectory_gradient_average: bfloat16 [4, 8, 1024, 4096], P('path', None, 'fsdp'), may hold values from -0.19921875 to 0.19921875
- trajectory_squared_average: bfloat16 [4, 8, 1024, 4096], P('path', None, 'fsdp'), may hold values from 0.0009994507 to 0.099609375
- common_expert_parameters: float32 [8, 2, 1024, 4096], P('path', None, 'fsdp'), may hold values from -6 to 6
- outer_inertia: float32 [8, 2, 1024, 4096], P('path', None, 'fsdp'), may hold values from -0.4 to 0.4
- trajectory_membership: int32 [4, 8], replicated, may hold values from 0 to 1
- punctual_flags: int32 [4], replicated, may hold values 0 or 1
Outputs:
- refreshed_experts: float32 [8, 2, 1024, 4096], P('path', None, 'fsdp')
- refreshed_inertia: float32 [8, 2, 1024, 4096], P('path', None, 'fsdp')
- returned: bfloat16 [4, 8, 1024, 4096], P('path', None, 'fsdp')
The draws below stay inside these ranges and needn't reach their ends.
All inputs are finite; a program needn't handle non-finite values.
Results may differ from the reference program's by a relative error of at most 0.0024.
Values may be sent and summed in bfloat16 or wider, within the bound.
A program may use at most 320 MiB of HBM per device.

```python
import math
import jax
import jax.numpy as jnp
from jax import lax

D = 2048
UNIT = 1024
SETS = 8
MPS = 2
STEP = 1000
TRAJECTORY_SUM = 4
TOKP = 1536


def touch_ends(array, own_key, smallest, largest):
    longest = array.shape.index(max(array.shape))
    spots = []
    for shift in (0, 1):
        where = [jax.random.randint(jax.random.fold_in(own_key, axis), (), 0, length) for axis, length in enumerate(array.shape)]
        where[longest] = (where[longest] + shift) % array.shape[longest]
        spots.append(tuple(where))
    return array.at[spots[0]].set(smallest).at[spots[1]].set(largest)


def block_levels(own_key, shape, pieces, smallest, largest):
    level = 1.0
    for position, parts in pieces:
        draws = jax.random.uniform(jax.random.fold_in(jax.random.fold_in(own_key, 6), position), (parts,), jnp.float32, smallest / len(pieces), largest / len(pieces))
        level = level * jnp.repeat(jnp.exp(draws), shape[position] // parts).reshape((-1,) + (1,) * (len(shape) - 1 - position))
    return level


def noise(key, shape, width, bound, shards=(), kind=jnp.bfloat16):
    level = block_levels(key, shape, shards, -0.22, 0.18) if shards else 1.0
    drawn = jax.random.normal(key, shape, jnp.float32) * width * level
    return jnp.minimum(jnp.maximum(drawn, -bound), bound).astype(kind)


def setup_inputs(seed: int = 0) -> dict:
    splits = jax.random.split(jax.random.key(seed), 10)
    input_activation_matrix = noise(splits[0], (TRAJECTORY_SUM, TOKP, D), 1.0, 6.0, ((0, 4), (1, 8)))
    output_sensitivity = noise(splits[1], (TRAJECTORY_SUM, TOKP, D), 2.0, 12.0, ((0, 4), (1, 8)))
    trajectory_initial_parameters = noise(splits[2], (TRAJECTORY_SUM, SETS, UNIT, 2 * D), 1.0, 6.0, ((0, 4), (2, 8)))
    trajectory_gradient_average = noise(splits[3], (TRAJECTORY_SUM, SETS, UNIT, 2 * D), 0.03, 0.19921875, ((0, 4), (2, 8)))
    trajectory_squared_average = jnp.clip(jnp.exp(math.log(0.099609375) - 4.6018058 * jax.random.uniform(splits[4], (TRAJECTORY_SUM, SETS, UNIT, 2 * D), jnp.float32) ** block_levels(splits[4], (TRAJECTORY_SUM, SETS, UNIT, 2 * D), ((0, 4), (2, 8)), -0.2, 0.2)), 0.0009994507, 0.099609375).astype(jnp.bfloat16)
    common_expert_parameters = noise(splits[5], (SETS, MPS, UNIT, 2 * D), 1.0, 6.0, ((0, 4), (2, 8)), jnp.float32)
    outer_inertia = noise(splits[6], (SETS, MPS, UNIT, 2 * D), 0.05, 0.4, ((0, 4), (2, 8)), jnp.float32)
    trajectory_membership = touch_ends(jax.random.randint(splits[7], (TRAJECTORY_SUM, SETS), 0, MPS), jax.random.fold_in(splits[7], 1), 0, MPS - 1).astype(jnp.int32)
    punctual_flags = touch_ends((jax.random.randint(splits[8], (TRAJECTORY_SUM,), 0, 2) < 1).astype(jnp.int32), jax.random.fold_in(splits[8], 1), 0, 1)
    return {"input_activation_matrix": input_activation_matrix, "output_sensitivity": output_sensitivity, "trajectory_initial_parameters": trajectory_initial_parameters, "trajectory_gradient_average": trajectory_gradient_average, "trajectory_squared_average": trajectory_squared_average, "common_expert_parameters": common_expert_parameters, "outer_inertia": outer_inertia, "trajectory_membership": trajectory_membership, "punctual_flags": punctual_flags}


BETA_ONE = 0.9
BETA_TWO = 0.999
ADAM_EPS = 1e-08
INNER_RATE = 0.05
DECAY = 0.1
GLOBAL_LEARNING = 0.7
INERTIA_FACTOR = 0.9

def adam_delta(grads, first, second, start):
    corr_one = 1.0 - BETA_ONE ** STEP
    corr_two = 1.0 - BETA_TWO ** STEP
    first_new = BETA_ONE * first.astype(jnp.float32) + (1.0 - BETA_ONE) * grads
    second_new = BETA_TWO * second.astype(jnp.float32) + (1.0 - BETA_TWO) * grads * grads
    direction = first_new / corr_one / (jnp.sqrt(second_new / corr_two) + ADAM_EPS)
    return (INNER_RATE * (direction + DECAY * start.astype(jnp.float32))).astype(jnp.bfloat16)

def path_grads(unit_rows, inputs, upstream):
    features = inputs.shape[1]
    in_rows = unit_rows[:, :features]
    out_rows = unit_rows[:, features:]
    input_scale = features ** (-0.5)
    hidden_scale = (SETS * UNIT) ** (-0.5)
    preact = jnp.dot(inputs, in_rows.T, preferred_element_type=jnp.float32) * input_scale
    active, pullback = jax.vjp(jax.nn.gelu, preact)
    active_half = active.astype(jnp.bfloat16)
    back_active = jnp.dot(upstream, out_rows.T, preferred_element_type=jnp.float32) * hidden_scale
    back_preact = pullback(back_active)[0].astype(jnp.bfloat16)
    grad_in = jnp.dot(back_preact.T, inputs, preferred_element_type=jnp.float32) * input_scale
    grad_out = jnp.dot(active_half.T, upstream, preferred_element_type=jnp.float32) * hidden_scale
    return jnp.concatenate([grad_in, grad_out], axis=1)

def reference(input_activation_matrix, output_sensitivity, trajectory_initial_parameters, trajectory_gradient_average, trajectory_squared_average, common_expert_parameters, outer_inertia, trajectory_membership, punctual_flags):
    eligible_trajectories = jnp.arange(MPS, dtype=jnp.int32)
    picked_trajectories = jnp.where((trajectory_membership[:, :, None] == eligible_trajectories[None, None, :]) & (punctual_flags[:, None, None] == 1), 1.0, 0.0).astype(jnp.float32)

    def accumulate(aggregate_change, items):
        inputs, upstream, start, first, second, weights = items
        unit_rows = start.reshape(SETS * UNIT, 2 * D)
        grads = path_grads(unit_rows, inputs, upstream)
        pseudo = adam_delta(grads, first.reshape(SETS * UNIT, 2 * D), second.reshape(SETS * UNIT, 2 * D), unit_rows)
        pseudo = pseudo.reshape(SETS, UNIT, 2 * D)
        return (aggregate_change + weights[:, :, None, None] * pseudo.astype(jnp.float32)[:, None], None)
    initial = jnp.zeros((SETS, MPS, UNIT, 2 * D), jnp.float32)
    aggregate_change, _ = lax.scan(accumulate, initial, (input_activation_matrix, output_sensitivity, trajectory_initial_parameters, trajectory_gradient_average, trajectory_squared_average, picked_trajectories))
    punctual_tally = lax.optimization_barrier(jnp.sum(picked_trajectories, axis=0))
    punctual_average = aggregate_change / jnp.maximum(punctual_tally, 1.0)[:, :, None, None]
    refreshed_inertia = INERTIA_FACTOR * outer_inertia + punctual_average
    refreshed_experts = common_expert_parameters - GLOBAL_LEARNING * (punctual_average + INERTIA_FACTOR * refreshed_inertia)
    updated = refreshed_experts.astype(jnp.bfloat16)
    set_index = jnp.arange(SETS, dtype=jnp.int32)
    returned = updated[set_index[None, :], trajectory_membership]
    return (refreshed_experts, refreshed_inertia, returned)
```

```python
import jax
import jax.numpy as jnp
from jax import lax
from jax.sharding import PartitionSpec as P

UNIT = 1024
SETS = 8
STEP = 1000


BETA_ONE = 0.9
BETA_TWO = 0.999
ADAM_EPS = 1e-08
INNER_RATE = 0.05
DECAY = 0.1
GLOBAL_LEARNING = 0.7
INERTIA_FACTOR = 0.9


def adam_delta(grads, first, second, start):
    corr_one = 1.0 - BETA_ONE**STEP
    corr_two = 1.0 - BETA_TWO**STEP
    first_new = BETA_ONE * first.astype(jnp.float32) + (1.0 - BETA_ONE) * grads
    second_new = BETA_TWO * second.astype(jnp.float32) + (1.0 - BETA_TWO) * grads * grads
    direction = first_new / corr_one / (jnp.sqrt(second_new / corr_two) + ADAM_EPS)
    return (INNER_RATE * (direction + DECAY * start.astype(jnp.float32))).astype(jnp.bfloat16)


def gather_tokens(block, step, size):
    pair = 2 - size % 2
    ring = size // pair
    swap = [(f, f ^ 1) for f in range(size)]
    turn = [(f, (f + pair * step) % size) for f in range(size)]
    chunks = []
    for index in range(ring):
        if pair == 2:
            chunks.append((block, lax.ppermute(block, "fsdp", swap)))
        else:
            chunks.append((block,))
        if index < ring - 1:
            block = lax.ppermute(block, "fsdp", turn)
    return chunks


def per_device(
    input_activation_matrix,
    output_sensitivity,
    trajectory_initial_parameters,
    trajectory_gradient_average,
    trajectory_squared_average,
    common_expert_parameters,
    outer_inertia,
    trajectory_membership,
    punctual_flags,
):
    set_count = trajectory_initial_parameters.shape[1]
    local_units = trajectory_initial_parameters.shape[2]
    row_width = trajectory_initial_parameters.shape[3]
    features = row_width // 2
    rows = set_count * local_units
    unit_rows = trajectory_initial_parameters[0].reshape(rows, row_width)
    in_rows = unit_rows[:, :features]
    out_rows = unit_rows[:, features:]
    input_scale = features ** (-0.5)
    hidden_scale = (SETS * UNIT) ** (-0.5)
    contract_last = (((1,), (1,)), ((), ()))
    contract_first = (((0,), (0,)), ((), ()))
    shards = lax.axis_size("fsdp")
    path_count = lax.axis_size("path")
    position = lax.axis_index("path")
    owned_sets = set_count // path_count
    choices = common_expert_parameters.shape[1]

    input_chunks = gather_tokens(input_activation_matrix[0], 1, shards)
    upstream_chunks = gather_tokens(output_sensitivity[0], 1, shards)

    tokens = input_activation_matrix.shape[1] * shards
    inputs = jnp.zeros((tokens, features), jnp.bfloat16)
    upstream = jnp.zeros((tokens, features), jnp.bfloat16)
    active = jnp.zeros((tokens, rows), jnp.bfloat16)
    back = jnp.zeros((tokens, rows), jnp.bfloat16)
    at = 0
    for x_blocks, g_blocks in zip(input_chunks, upstream_chunks):
        for x_block, g_block in zip(x_blocks, g_blocks):
            preact = (
                lax.dot_general(
                    x_block, in_rows, contract_last, preferred_element_type=jnp.float32
                )
                * input_scale
            )
            act, pullback = jax.vjp(jax.nn.gelu, preact)
            back_active = (
                lax.dot_general(
                    g_block, out_rows, contract_last, preferred_element_type=jnp.float32
                )
                * hidden_scale
            )
            dpre = pullback(back_active)[0].astype(jnp.bfloat16)
            inputs = lax.dynamic_update_slice(inputs, x_block, (at, 0))
            upstream = lax.dynamic_update_slice(upstream, g_block, (at, 0))
            active = lax.dynamic_update_slice(active, act.astype(jnp.bfloat16), (at, 0))
            back = lax.dynamic_update_slice(back, dpre, (at, 0))
            at += x_block.shape[0]

    owned_rows = owned_sets * local_units

    def moments(array, owner):
        return lax.dynamic_slice_in_dim(array[0], owner * owned_sets, owned_sets, 0).reshape(
            owned_rows, row_width
        )

    def pseudo_for(owner):
        start = moments(trajectory_initial_parameters, owner)
        first = moments(trajectory_gradient_average, owner)
        second = moments(trajectory_squared_average, owner)
        back_own = lax.dynamic_slice_in_dim(back, owner * owned_rows, owned_rows, 1)
        active_own = lax.dynamic_slice_in_dim(active, owner * owned_rows, owned_rows, 1)
        grad_in = (
            lax.dot_general(back_own, inputs, contract_first, preferred_element_type=jnp.float32)
            * input_scale
        )
        grad_out = (
            lax.dot_general(
                active_own, upstream, contract_first, preferred_element_type=jnp.float32
            )
            * hidden_scale
        )
        halves = [
            adam_delta(grad, first[:, cut], second[:, cut], start[:, cut])
            for grad, cut in (
                (grad_in, slice(0, features)),
                (grad_out, slice(features, row_width)),
            )
        ]
        return jnp.concatenate(halves, axis=1).reshape(owned_sets, local_units, row_width)

    hops = list(range(path_count - 1, 0, -1))
    trade = {k: [(p, p ^ k) for p in range(path_count)] for k in hops}
    arrived = {}
    for k in hops + [0]:
        pseudo = pseudo_for(position ^ k)
        for j in range(owned_sets):
            piece = pseudo[j]
            arrived[k, j] = piece if k == 0 else lax.ppermute(piece, "path", trade[k])

    eligible_trajectories = jnp.arange(choices, dtype=jnp.int32)
    picked_trajectories = jnp.where(
        (trajectory_membership[:, :, None] == eligible_trajectories[None, None, :])
        & (punctual_flags[:, None, None] == 1),
        1.0,
        0.0,
    ).astype(jnp.float32)
    first_set = position * owned_sets
    owner_weights = lax.dynamic_slice_in_dim(picked_trajectories, first_set, owned_sets, 1)
    owner_choice = lax.dynamic_slice_in_dim(trajectory_membership, first_set, owned_sets, 1)
    tally = jnp.maximum(jnp.sum(owner_weights, axis=0), 1.0)
    weights = {
        k: lax.dynamic_index_in_dim(owner_weights, position ^ k, 0, keepdims=False)
        for k in hops + [0]
    }
    wanted = {
        k: lax.dynamic_index_in_dim(owner_choice, position ^ k, 0, keepdims=False)
        for k in hops + [0]
    }

    experts, inertias = [], []
    returned = jnp.zeros((set_count, local_units, row_width), jnp.bfloat16)
    for j in range(owned_sets):
        total = sum(
            weights[k][j][:, None, None] * arrived[k, j].astype(jnp.float32)[None]
            for k in hops + [0]
        )
        average = total / tally[j][:, None, None]
        inertia = INERTIA_FACTOR * outer_inertia[j] + average
        expert = common_expert_parameters[j] - GLOBAL_LEARNING * (
            average + INERTIA_FACTOR * inertia
        )
        experts.append(expert)
        inertias.append(inertia)
        updated = expert.astype(jnp.bfloat16)
        for k in hops + [0]:
            chosen = updated[0]
            for c in range(1, choices):
                chosen = jnp.where(wanted[k][j] == c, updated[c], chosen)
            if k:
                chosen = lax.ppermute(chosen, "path", trade[k])
            returned = lax.dynamic_update_slice(
                returned, chosen[None], ((position ^ k) * owned_sets + j, 0, 0)
            )
    return (jnp.stack(experts), jnp.stack(inertias), returned[None])


def solution(mesh):
    placed = (
        P("path", "fsdp", None),
        P("path", "fsdp", None),
        P("path", None, "fsdp", None),
        P("path", None, "fsdp", None),
        P("path", None, "fsdp", None),
        P("path", None, "fsdp", None),
        P("path", None, "fsdp", None),
        P(),
        P(),
    )
    return jax.shard_map(
        per_device,
        mesh=mesh,
        in_specs=placed,
        out_specs=(
            P("path", None, "fsdp", None),
            P("path", None, "fsdp", None),
            P("path", None, "fsdp", None),
        ),
        check_vma=False,
    )
```
